32 devices in a mesh: tm: 8 (over z, y), space: 4 (over x, core).
Axes of the slice: x: 2, y: 2, z: 4, core: 2. Of those that a mesh axis runs over, the one named last changes fastest.
Arguments:
- observed: float32 [64, 512, 128], P('tm', 'space'), may hold values from -6 to 6
- gain: float32 [4, 128, 128], P('space'), may hold values from -0.15625 to 0.15625
- trans: float32 [4, 384, 128], P('space'), may hold values from -1 to 1
- dynamics: float32 [4, 384, 128], P('space'), may hold values from -1 to 1
- smooth_gain: float32 [4, 384, 128], P('space'), may hold values from -1 to 1
Outputs:
- filtered: float32 [64, 512, 128], P('tm', 'space')
- smoothed: float32 [64, 512, 128], P('tm', 'space')
The draws below stay inside these ranges and needn't reach their ends.
All inputs are finite; a program needn't handle non-finite values.
Results may differ from the reference program's by a relative error of at most 0.00017.
Values sent between devices are 32-bit elements; how exact they have to be, the bound alone decides.
A program may use at most 128 MiB of HBM per device.

```python
import jax
import jax.numpy as jnp
from jax import lax

TILE = 128
MEMBERS = 128
STEPS = 64
STATE = 512
N_SPACE = 4


def banded_draw(key, slow_share):
    count_tiles = STATE // TILE
    key_noise, key_rate, key_pick = jax.random.split(key, 3)
    noise = jax.random.normal(key_noise, (count_tiles, 3 * TILE, TILE), jnp.float32) * (0.05 / (3 * TILE))
    picks = jax.random.uniform(key_pick, (count_tiles, TILE), jnp.float32)
    levels = jax.random.uniform(key_rate, (count_tiles, TILE), jnp.float32)
    slow = 0.993 + 0.005 * levels
    fast = 0.5 + 0.45 * levels
    rates = jnp.where(picks < slow_share, slow, fast)
    diagonal = jnp.eye(TILE, dtype=jnp.float32)[None] * rates[:, None, :]
    coupling = 0.25
    upper = noise[:, :TILE, :] + coupling * diagonal
    middle = noise[:, TILE:2 * TILE, :] + (1.0 - 2.0 * coupling) * diagonal
    lower = noise[:, 2 * TILE:, :] + coupling * diagonal
    return jnp.concatenate([upper, middle, lower], 1)


def draw_trans(key, part):
    return banded_draw(jax.random.fold_in(key, 11), 0.5)


def draw_dynamics(key, part):
    return banded_draw(jax.random.fold_in(key, 23), 0.5)


def draw_smooth_gain(key, part):
    return banded_draw(jax.random.fold_in(key, 37), 0.5)


def level_of(stream_key, dims, cuts, smallest, high):
    def one(dim, shards_of):
        draws = jax.random.uniform(jax.random.fold_in(jax.random.fold_in(stream_key, 6), dim), (shards_of,), jnp.float32, smallest / len(cuts), high / len(cuts))
        return jnp.repeat(jnp.exp(draws), dims[dim] // shards_of).reshape((-1,) + (1,) * (len(dims) - dim - 1))

    level = one(*cuts[0])
    for cut in cuts[1:]:
        level = level * one(*cut)
    return level


def scatter_about(rng, dims, scale, most, cuts=(), held_as=jnp.bfloat16):
    array = jax.random.normal(rng, dims, jnp.float32) * scale
    if len(cuts) > 0:
        array = level_of(rng, dims, cuts, -0.22, 0.18) * array
    return jnp.clip(array, min=-most, max=most).astype(held_as)


def setup_inputs(seed: int = 0) -> dict:
    seeds = jax.random.split(jax.random.key(seed), 6)
    return {
        "observed": scatter_about(seeds[0], (STEPS, STATE, MEMBERS), 1.0, 6.0, ((0, 8), (1, 4)), jnp.float32),
        "gain": scatter_about(seeds[1], (N_SPACE, TILE, TILE), (10 * TILE) ** -0.5, 0.15625, ((0, 4),), jnp.float32),
        "trans": draw_trans(jax.random.fold_in(seeds[5], 71), 0),
        "dynamics": draw_dynamics(jax.random.fold_in(seeds[5], 71), 0),
        "smooth_gain": draw_smooth_gain(jax.random.fold_in(seeds[5], 71), 0),
    }


highest_mode = lax.Precision.HIGHEST


def apply_band(banded, current):
    count_tiles = banded.shape[0]
    tile_width = banded.shape[2]
    blocks = current.reshape(current.shape[0], count_tiles, tile_width, current.shape[2])
    empty_tile = jnp.zeros_like(blocks[:, :1])
    padded = jnp.concatenate([empty_tile, blocks, empty_tile], 1)
    stacked = jnp.concatenate([padded[:, :-2], padded[:, 1:-1], padded[:, 2:]], 2)
    result = jnp.einsum("crs,ncre->ncse", banded, stacked, precision=highest_mode)
    return result.reshape(current.shape)


def reference(observed, gain, trans, dynamics, smooth_gain):
    count_tiles = gain.shape[0]
    tile_width = gain.shape[1]
    steps = observed.shape[0]
    members = observed.shape[2]
    blocks = observed.reshape(steps, count_tiles, tile_width, members)
    forcing = jnp.einsum("cos,tcoe->tcse", gain, blocks, precision=highest_mode).reshape(observed.shape)

    def forward(carry, force):
        current = apply_band(trans, carry[None])[0] + force
        return current, current

    start = jnp.zeros(observed.shape[1:], jnp.float32)
    final_state, filtered = lax.scan(forward, start, forcing)
    mixed = apply_band(smooth_gain, apply_band(dynamics, filtered))
    innovation = jnp.concatenate([(filtered - mixed)[:-1], filtered[-1:]], 0)

    def backward(carry, drive):
        current = apply_band(smooth_gain, carry[None])[0] + drive
        return current, current

    first_state, smoothed = lax.scan(backward, start, innovation, reverse=True)
    return filtered, smoothed
```

```python
from functools import partial

import jax
import jax.numpy as jnp
from jax import lax
from jax.experimental import pallas as pl
from jax.experimental.pallas import tpu as pltpu
from jax.sharding import PartitionSpec as P

highest_mode = lax.Precision.HIGHEST


def shifted(shard, axis, by):
    devices = lax.axis_size(axis)
    pairs = [(i, i + by) for i in range(devices) if 0 <= i + by < devices]
    return lax.ppermute(shard, axis, pairs)


def apply_full(banded, current):
    count_tiles = banded.shape[0]
    tile_width = banded.shape[2]
    blocks = current.reshape(current.shape[0], count_tiles, tile_width, current.shape[2])
    empty_tile = jnp.zeros_like(blocks[:, :1])
    padded = jnp.concatenate([empty_tile, blocks, empty_tile], 1)
    stacked = jnp.concatenate([padded[:, :-2], padded[:, 1:-1], padded[:, 2:]], 2)
    result = jnp.einsum("crs,ncre->ncse", banded, stacked, precision=highest_mode)
    return result.reshape(current.shape)


def sweep(apply_step, inputs, entry, backward):
    length = inputs.shape[0]
    order = list(range(length - 1, -1, -1)) if backward else list(range(length))
    current = entry
    outputs = [entry] * length
    for moment in order:
        current = apply_step(current[None])[0] + inputs[moment]
        outputs[moment] = current
    return jnp.stack(outputs)


def carry_prefix(carry, tables, which, direction):
    total = carry
    for level in range(len(tables) + 1):
        reach = direction * (1 if level == 0 else 2 ** (level - 1))
        moved = shifted(total, "tm", reach)
        if level == 0:
            total = moved
        else:
            table = tables[level - 1][which]

            def term(start, count, table=table, moved=moved):
                return lax.dot_general(
                    table, moved, (((0,), (0,)), ((), ())), precision=highest_mode
                )

            total = total + lax.psum_scatter(
                term(jnp.int32(0), moved.shape[0] * lax.axis_size("space")),
                "space",
                scatter_dimension=0,
                tiled=True,
            )
    return total


def body(observed, gain, trans, dynamics, smooth_gain):
    steps, tile_width, members = observed.shape
    count_tiles = lax.axis_size("space")
    ranks = lax.axis_size("tm")
    place = lax.axis_index("tm")
    column = lax.axis_index("space")
    state_width = tile_width * count_tiles
    block_cols = state_width // ranks
    sections = (ranks - 1).bit_length()
    log_steps = steps.bit_length() - 1
    forcing = jnp.einsum("os,toe->tse", gain[0], observed, precision=highest_mode)
    full_trans, full_smooth, full_dynamics = (
        lax.all_gather(trans, "space", axis=0, tiled=True),
        lax.all_gather(smooth_gain, "space", axis=0, tiled=True),
        lax.all_gather(dynamics, "space", axis=0, tiled=True),
    )

    def first_block(full):
        target = place * block_cols // tile_width
        offset = place * block_cols % tile_width
        index = jnp.clip(target, 0, full.shape[0] - 1)
        slab = lax.dynamic_index_in_dim(full, index, 0, keepdims=False)
        row_start = jnp.clip(column - target + 1, 0, 2) * tile_width
        piece = lax.dynamic_slice(slab, (row_start, offset), (tile_width, block_cols))
        inside = (jnp.abs(column - target) <= 1).astype(jnp.float32)
        return piece * inside

    blocks = (first_block(full_trans), first_block(full_smooth))
    needed = []
    for level in range(log_steps + sections - 1):
        col_trans = lax.all_gather(blocks[0], "space", axis=0, tiled=True)
        col_smooth = lax.all_gather(blocks[1], "space", axis=0, tiled=True)
        blocks = (
            jnp.dot(
                lax.all_gather(blocks[0], "tm", axis=1, tiled=True),
                col_trans,
                precision=highest_mode,
            ),
            jnp.dot(
                lax.all_gather(blocks[1], "tm", axis=1, tiled=True),
                col_smooth,
                precision=highest_mode,
            ),
        )
        if level + 1 >= log_steps:
            needed.append(blocks)
    tables = []
    for pair in needed:
        tables.append(
            (
                lax.all_gather(pair[0], "tm", axis=1, tiled=True),
                lax.all_gather(pair[1], "tm", axis=1, tiled=True),
            )
        )
    final_moment = jnp.arange(steps)[:, None, None] == steps - 1
    at_end = jnp.logical_and(final_moment, place == ranks - 1)
    whole_forcing = lax.all_gather(forcing, "space", axis=1, tiled=True)
    zero_full = jnp.zeros((state_width, members), jnp.float32)
    step_trans = partial(apply_full, full_trans)
    step_smooth = partial(apply_full, full_smooth)
    trial = sweep(step_trans, whole_forcing, zero_full, False)
    own_tail = lax.dynamic_slice_in_dim(trial[steps - 1], column * tile_width, tile_width, 0)
    entry = carry_prefix(own_tail, tables, 0, 1)
    entry_full = lax.all_gather(entry, "space", axis=0, tiled=True)
    filtered_full = sweep(step_trans, whole_forcing, entry_full, False)
    mixed_full = apply_full(full_smooth, apply_full(full_dynamics, filtered_full))
    innovation_full = jnp.where(at_end, filtered_full, filtered_full - mixed_full)
    trial_back = sweep(step_smooth, innovation_full, zero_full, True)
    own_head = lax.dynamic_slice_in_dim(trial_back[0], column * tile_width, tile_width, 0)
    exit_state = carry_prefix(own_head, tables, 1, -1)
    exit_full = lax.all_gather(exit_state, "space", axis=0, tiled=True)
    smoothed_full = sweep(step_smooth, innovation_full, exit_full, True)
    filtered = lax.dynamic_slice_in_dim(filtered_full, column * tile_width, tile_width, 1)
    smoothed = lax.dynamic_slice_in_dim(smoothed_full, column * tile_width, tile_width, 1)
    return (filtered, smoothed)

MESH = pl.DeviceIdType.MESH
SUBLANES = 8
SPLIT = (0, 1, 2)


def pieces(x):
    high = x.astype(jnp.bfloat16)
    return high, (x - high.astype(jnp.float32)).astype(jnp.bfloat16)


def dot(a, b):
    return jnp.dot(a, b, preferred_element_type=jnp.float32)


def times(x, table):
    rows = x.shape[0]
    high = x.astype(jnp.bfloat16).astype(jnp.float32)
    both = jnp.concatenate([high, x - high], 0).astype(jnp.bfloat16)
    two = dot(both, table[0])
    return two[:rows] + (two[rows:] + dot(both[:rows], table[1]))


def product(left, right, result):
    width = left.shape[1]
    part = min(width, 256)
    for start in range(0, width, part):
        rows = slice(start, start + part)
        high, low = left[0, rows, :], left[1, rows, :]
        two = dot(jnp.concatenate([high, low], 0), right[0])
        total = two[:part] + (two[part:] + dot(high, right[1]))
        for place, piece in enumerate(pieces(total)):
            result[place, rows, :] = piece


def kernel(
    ranks, columns, observed, gain, trans, dynamics, smooth_gain, filtered, smoothed,
    outbox, forcing, states, drive, results, inbox_f, inbox_s, ends, sums, firsts, edge, carry, raw,
    trans_1, trans_2, trans_4, trans_8, smooth_1, smooth_2, smooth_4, smooth_8, dyn_1, mix_1,
    table_send, table_recv, table_own, force_send, force_recv, filt_send, filt_recv, smoo_send, smoo_recv,
    carry_send, carry_recv, own_sem,
):
    steps, tile_width, members = observed.shape
    short = steps // 2
    span = ranks // 2
    group = span * columns
    subs = 2 * span
    rows = subs * SUBLANES
    state_width = columns * tile_width
    rank = lax.axis_index("tm")
    column = lax.axis_index("space")
    half = rank // span
    local = rank % span
    me = local * columns + column
    beside = column + 1 - 2 * (column % 2)
    across = (column + 2) % columns
    early = half == 0
    late = half == 1

    barrier = pltpu.get_barrier_semaphore()

    def member(offset):
        other = (me + offset) % group
        return other // columns, other % columns

    def greet(offset, _):
        place, lane = member(offset)
        pl.semaphore_signal(
            barrier, inc=1, device_id=(half * span + place, lane), device_id_type=MESH
        )
        return 0

    lax.fori_loop(1, group, greet, 0)
    opposite = (rank + span) % ranks
    pl.semaphore_signal(barrier, inc=1, device_id=(opposite, column), device_id_type=MESH)

    sources = (trans, smooth_gain, dynamics)
    for which, source in enumerate(sources):
        pltpu.make_async_copy(source.at[0], raw.at[which, column], table_own.at[which]).start()

    gain_high, gain_low = pieces(gain[0])

    def force(step, _):
        for part in range(2):
            image = observed[part * short + step].T
            high, low = pieces(image)
            value = dot(high, gain_high) + (dot(low, gain_high) + dot(high, gain_low))
            outbox[:, pl.ds(step, 1), part] = value.reshape(group, 1, SUBLANES, tile_width)
        return 0

    lax.fori_loop(0, short, force, 0)
    pl.semaphore_wait(barrier, group)

    shared = rank % 2
    partner = rank + 1 - 2 * shared

    def half_rows(index):
        count = 3 * tile_width // 2
        return pl.ds(pl.multiple_of(index * count, count), count)

    def table_copy(which, what):
        split = which in SPLIT
        if what == 0:
            place, to = column, (rank, across)
            part = half_rows(shared) if split else slice(None)
        elif what == 1:
            place, to, part = column, (rank, beside), slice(None)
        elif what == 2:
            place, to = across, (rank, beside)
            part = half_rows(shared) if split else slice(None)
        elif what == 3:
            place, to, part = across, (partner, column), half_rows(shared)
        else:
            place, to, part = across, (rank, beside), half_rows(1 - shared)
        source = sources[which].at[0, part] if what < 2 else raw.at[which, place, part]
        return pltpu.make_async_remote_copy(
            src_ref=source,
            dst_ref=raw.at[which, place, part],
            send_sem=table_send.at[which, what],
            recv_sem=table_recv.at[which, what],
            device_id=to,
            device_id_type=MESH,
        )

    def send_table(which):
        table_copy(which, 0).start()
        table_copy(which, 1).start()

    def relay_table(which):
        table_copy(which, 0).wait_recv()
        if which in SPLIT:
            table_copy(which, 3).start()
        table_copy(which, 2).start()

    def relay_again(which):
        if which in SPLIT:
            table_copy(which, 3).wait_recv()
            table_copy(which, 4).start()

    def finish_table(which):
        pltpu.make_async_copy(sources[which].at[0], raw.at[which, column], table_own.at[which]).wait()
        table_copy(which, 1).wait_recv()
        table_copy(which, 2).wait_recv()
        if which in SPLIT:
            table_copy(which, 4).wait_recv()

    def build(which, table):
        for tile in range(columns):
            lanes = slice(tile * tile_width, (tile + 1) * tile_width)
            for row in range(columns):
                part = slice(row * tile_width, (row + 1) * tile_width)
                shift = row - tile + 1
                if 0 <= shift <= 2:
                    block = raw[which, tile, shift * tile_width : (shift + 1) * tile_width, :]
                    for place, piece in enumerate(pieces(block)):
                        table[place, part, lanes] = piece
                else:
                    for place in range(2):
                        table[place, part, lanes] = jnp.zeros((tile_width, tile_width), jnp.bfloat16)

    def lane_part(index):
        return pl.ds(pl.multiple_of(index * tile_width, tile_width), tile_width)

    def force_copy(offset):
        place, lane = member(offset)
        return pltpu.make_async_remote_copy(
            src_ref=outbox.at[(me + offset) % group],
            dst_ref=forcing.at[:, pl.ds(2 * local, 2), :, lane_part(column)],
            send_sem=force_send.at[offset],
            recv_sem=force_recv.at[offset],
            device_id=(half * span + place, lane),
            device_id_type=MESH,
        )

    def result_copy(offset, source, inbox, send, recv):
        place, lane = member(offset)
        return pltpu.make_async_remote_copy(
            src_ref=source.at[:, pl.ds(2 * place, 2), :, lane_part(lane)],
            dst_ref=inbox.at[me],
            send_sem=send.at[offset],
            recv_sem=recv.at[offset],
            device_id=(half * span + place, lane),
            device_id_type=MESH,
        )

    def own_result(source, inbox, index):
        return pltpu.make_async_copy(
            source.at[:, pl.ds(2 * local, 2), :, lane_part(column)], inbox.at[me], own_sem.at[index]
        )

    def carry_copy(index):
        return pltpu.make_async_remote_copy(
            src_ref=edge.at[index],
            dst_ref=carry.at[index],
            send_sem=carry_send.at[index],
            recv_sem=carry_recv.at[index],
            device_id=(opposite, column),
            device_id_type=MESH,
        )

    def over_others(act):
        def one(offset, _):
            act(offset)
            return 0

        lax.fori_loop(1, group, one, 0)

    filtered_copy = lambda offset: result_copy(offset, states, inbox_f, filt_send, filt_recv)
    smoothed_copy = lambda offset: result_copy(offset, results, inbox_s, smoo_send, smoo_recv)

    send_table(0)
    over_others(lambda offset: force_copy(offset).start())
    own_force = pltpu.make_async_copy(
        outbox.at[me], forcing.at[:, pl.ds(2 * local, 2), :, lane_part(column)], own_sem.at[0]
    )
    own_force.start()
    send_table(1)
    send_table(2)

    relay_table(0)
    relay_again(0)
    finish_table(0)
    build(0, trans_1)
    product(trans_1, trans_1, trans_2)
    product(trans_2, trans_2, trans_4)
    product(trans_4, trans_4, trans_8)
    over_others(lambda offset: force_copy(offset).wait_recv())
    own_force.wait()

    def flat(x):
        return x.reshape(-1, state_width)

    def pairs(x):
        both = x.reshape(span, 2, SUBLANES, state_width)
        return both[:, 0], both[:, 1]

    def stacked(first, second):
        return jnp.stack([first, second], 1).reshape(rows, state_width)

    def relays():
        relay_table(1)
        relay_table(2)
        relay_again(1)
        relay_again(2)

    def smooth_tables():
        finish_table(1)
        build(1, smooth_1)
        product(smooth_1, smooth_1, smooth_2)
        product(smooth_2, smooth_2, smooth_4)
        product(smooth_4, smooth_4, smooth_8)
        finish_table(2)
        build(2, dyn_1)
        product(dyn_1, smooth_1, mix_1)

    @pl.when(late)
    def _():
        relays()

    current = flat(forcing[0])
    for step in range(1, short):
        current = times(current, trans_1) + flat(forcing[step])
    ends[...] = current.reshape(ends.shape)
    even, odd = pairs(current)
    sums[...] = times(flat(even), trans_4).reshape(sums.shape) + odd

    @pl.when(early)
    def _():
        firsts[0] = jnp.zeros_like(firsts[0])
        state = sums[0]
        for index in range(1, span):
            firsts[index] = state
            state = times(state, trans_8) + sums[index]
        edge[0] = state
        carry_copy(0).start()
        relays()

    @pl.when(late)
    def _():
        smooth_tables()
        carry_copy(0).wait_recv()
        state = carry[0]
        firsts[0] = state
        for index in range(1, span):
            state = times(state, trans_8) + sums[index - 1]
            firsts[index] = state

    even, _ = pairs(ends[...])
    first = firsts[...]
    second = times(flat(first), trans_4).reshape(sums.shape) + even
    current = stacked(first, second)
    for step in range(short):
        current = times(current, trans_1) + flat(forcing[step])
        states[step] = current.reshape(ends.shape)

    over_others(lambda offset: filtered_copy(offset).start())
    own_result(states, inbox_f, 1).start()

    @pl.when(early)
    def _():
        smooth_tables()

    for step in range(short):
        value = flat(states[step])
        mixed = times(value, mix_1)
        if step == short - 1:
            place = lax.broadcasted_iota(jnp.int32, mixed.shape, 0)
            at_end = jnp.logical_and(place >= rows - SUBLANES, late)
            mixed = jnp.where(at_end, jnp.zeros_like(mixed), mixed)
        drive[step] = (value - mixed).reshape(ends.shape)

    current = flat(drive[short - 1])
    for step in range(short - 2, -1, -1):
        current = times(current, smooth_1) + flat(drive[step])
    ends[...] = current.reshape(ends.shape)
    even, odd = pairs(current)
    sums[...] = times(flat(odd), smooth_4).reshape(sums.shape) + even

    @pl.when(late)
    def _():
        firsts[span - 1] = jnp.zeros_like(firsts[0])
        state = sums[span - 1]
        for index in range(span - 2, -1, -1):
            firsts[index] = state
            state = times(state, smooth_8) + sums[index]
        edge[1] = state
        carry_copy(1).start()

    @pl.when(early)
    def _():
        carry_copy(1).wait_recv()
        state = carry[1]
        firsts[span - 1] = state
        for index in range(span - 2, -1, -1):
            state = times(state, smooth_8) + sums[index + 1]
            firsts[index] = state

    _, odd = pairs(ends[...])
    last = firsts[...]
    before = times(flat(last), smooth_4).reshape(sums.shape) + odd
    current = stacked(before, last)
    for step in range(short - 1, -1, -1):
        current = times(current, smooth_1) + flat(drive[step])
        results[step] = current.reshape(ends.shape)

    over_others(lambda offset: smoothed_copy(offset).start())
    own_result(results, inbox_s, 2).start()

    def deliver(inbox, output):
        def one(step, _):
            for part in range(2):
                block = inbox[:, pl.ds(step, 1), part].reshape(members, tile_width)
                output[part * short + step] = block.T
            return 0

        lax.fori_loop(0, short, one, 0)

    over_others(lambda offset: filtered_copy(offset).wait_recv())
    own_result(states, inbox_f, 1).wait()
    deliver(inbox_f, filtered)
    over_others(lambda offset: smoothed_copy(offset).wait_recv())
    own_result(results, inbox_s, 2).wait()
    deliver(inbox_s, smoothed)

    for which in range(3):
        for what in range(5 if which in SPLIT else 3):
            table_copy(which, what).wait_send()
    over_others(lambda offset: force_copy(offset).wait_send())
    over_others(lambda offset: filtered_copy(offset).wait_send())
    over_others(lambda offset: smoothed_copy(offset).wait_send())

    @pl.when(early)
    def _():
        carry_copy(0).wait_send()

    @pl.when(late)
    def _():
        carry_copy(1).wait_send()


def member_body(ranks, columns, observed, gain, trans, dynamics, smooth_gain):
    steps, tile_width, members = observed.shape
    short = steps // 2
    span = ranks // 2
    group = span * columns
    width = columns * tile_width
    boxes = pltpu.VMEM((group, short, 2, SUBLANES, tile_width), jnp.float32)
    series = pltpu.VMEM((short, 2 * span, SUBLANES, width), jnp.float32)
    block = pltpu.VMEM((2 * span, SUBLANES, width), jnp.float32)
    small = pltpu.VMEM((span, SUBLANES, width), jnp.float32)
    edges = pltpu.VMEM((2, SUBLANES, width), jnp.float32)
    table = pltpu.VMEM((2, width, width), jnp.bfloat16)
    each = pltpu.SemaphoreType.DMA((group,))
    vmem = pl.BlockSpec(memory_space=pltpu.VMEM)
    return pl.pallas_call(
        partial(kernel, ranks, columns),
        out_shape=[jax.ShapeDtypeStruct(observed.shape, jnp.float32)] * 2,
        in_specs=[vmem] * 5,
        out_specs=[vmem] * 2,
        scratch_shapes=[
            boxes, series, series, series, series, boxes, boxes, block, small, small, edges, edges,
            pltpu.VMEM((3, columns, 3 * tile_width, tile_width), jnp.float32),
            table, table, table, table, table, table, table, table, table, table,
            pltpu.SemaphoreType.DMA((3, 5)),
            pltpu.SemaphoreType.DMA((3, 5)),
            pltpu.SemaphoreType.DMA((3,)),
            each, each, each, each, each, each,
            pltpu.SemaphoreType.DMA((2,)),
            pltpu.SemaphoreType.DMA((2,)),
            pltpu.SemaphoreType.DMA((3,)),
        ],
        compiler_params=pltpu.CompilerParams(
            collective_id=0, has_side_effects=True, vmem_limit_bytes=56 * 2**20
        ),
    )(observed, gain, trans, dynamics, smooth_gain)


def by_members(mesh, observed, gain, trans, dynamics, smooth_gain):
    ranks, columns = mesh.shape["tm"], mesh.shape["space"]
    steps, tile_width, members = observed.shape
    fits = (
        ranks % 2 == 0
        and ranks >= 4
        and members == ranks // 2 * columns * SUBLANES
        and steps % 2 == 0
        and steps >= 4
        and columns == 4
        and tile_width == 128
        and members == 128
    )
    if fits:
        return tuple(member_body(ranks, columns, observed, gain, trans, dynamics, smooth_gain))
    return body(observed, gain, trans, dynamics, smooth_gain)


def solution(mesh):
    return jax.shard_map(
        partial(by_members, mesh),
        mesh=mesh,
        in_specs=(
            P("tm", "space", None),
            P("space", None, None),
            P("space", None, None),
            P("space", None, None),
            P("space", None, None),
        ),
        out_specs=(P("tm", "space", None), P("tm", "space", None)),
        check_vma=False,
    )
```
